16 devices in a mesh: tp: 2 (over z), fsdp: 8 (over y, x, core).
Axes of the slice: x: 2, y: 2, z: 2, core: 2. Of those that a mesh axis runs over, the one named last changes fastest.
Arguments:
- patches: bfloat16 [256, 49, 3072], P('fsdp')
- labels: int32 [256], P('fsdp')
- w_stem: float32 [3072, 1024], P('fsdp', 'tp')
- b_stem: float32 [1024], P(('tp', 'fsdp'))
- ln1_g: float32 [2, 1024], P(None, ('tp', 'fsdp'))
- ln1_b: float32 [2, 1024], P(None, ('tp', 'fsdp'))
- w_tok1: float32 [2, 49, 512], P(None, None, 'fsdp')
- b_tok1: float32 [2, 512], P(None, 'fsdp')
- w_tok2: float32 [2, 512, 49], P(None, 'fsdp')
- ln2_g: float32 [2, 1024], P(None, ('tp', 'fsdp'))
- ln2_b: float32 [2, 1024], P(None, ('tp', 'fsdp'))
- w_ch1: float32 [2, 1024, 4096], P(None, 'fsdp', 'tp')
- b_ch1: float32 [2, 4096], P(None, ('tp', 'fsdp'))
- w_ch2: float32 [2, 4096, 1024], P(None, ('tp', 'fsdp'))
- b_ch2: float32 [2, 1024], P(None, ('tp', 'fsdp'))
- lnf_g: float32 [1024], P(('tp', 'fsdp'))
- lnf_b: float32 [1024], P(('tp', 'fsdp'))
- w_head: float32 [1024, 1000], P('fsdp', 'tp')
- b_head: float32 [1000], P('tp')
Outputs:
- output 1: float32 [], replicated
- output 2: float32 [3072, 1024], P('fsdp', 'tp')
- output 3: float32 [1024], P(('tp', 'fsdp'))
- output 4: float32 [2, 1024], P(None, ('tp', 'fsdp'))
- output 5: float32 [2, 1024], P(None, ('tp', 'fsdp'))
- output 6: float32 [2, 49, 512], P(None, None, 'fsdp')
- output 7: float32 [2, 512], P(None, 'fsdp')
- output 8: float32 [2, 512, 49], P(None, 'fsdp')
- output 9: float32 [2, 1024], P(None, ('tp', 'fsdp'))
- output 10: float32 [2, 1024], P(None, ('tp', 'fsdp'))
- output 11: float32 [2, 1024, 4096], P(None, 'fsdp', 'tp')
- output 12: float32 [2, 4096], P(None, ('tp', 'fsdp'))
- output 13: float32 [2, 4096, 1024], P(None, ('tp', 'fsdp'))
- output 14: float32 [2, 1024], P(None, ('tp', 'fsdp'))
- output 15: float32 [1024], P(('tp', 'fsdp'))
- output 16: float32 [1024], P(('tp', 'fsdp'))
- output 17: float32 [1024, 1000], P('fsdp', 'tp')
- output 18: float32 [1000], P('tp')
All inputs are finite; a program needn't handle non-finite values.
Results may differ from the reference program's by a relative error of at most 0.0162012.
Values are sent between devices in bfloat16 or wider.
A program may use at most 1 GiB of HBM per device.

```python
import jax
import jax.numpy as jnp
from jax import lax

PATCH_SIDE = 32
TOKENS = 49
CHANNELS = 1024
TOKEN_HIDDEN = 512
CHANNEL_HIDDEN = 4096
CLASSES = 1000
LAYERS = 2
IMAGES = 256
BLOCKS = 8

PATCH_DIM = 3 * PATCH_SIDE * PATCH_SIDE
PER_BLOCK = IMAGES // BLOCKS
EPS = 1e-6
LAYER_NAMES = ('ln1_g', 'ln1_b', 'w_tok1', 'b_tok1', 'w_tok2', 'ln2_g', 'ln2_b', 'w_ch1', 'b_ch1', 'w_ch2', 'b_ch2')


def setup_inputs(seed: int = 0) -> dict:
    key_list = jax.random.split(jax.random.key(seed), 20)

    def normal(index, shape, scale):
        return scale * jax.random.normal(key_list[index], shape, jnp.float32)

    chan_shape = (LAYERS, CHANNELS)
    return {
        'patches': normal(0, (IMAGES, TOKENS, PATCH_DIM), 1.0).astype(jnp.bfloat16),
        'labels': jax.random.randint(key_list[1], (IMAGES,), 0, CLASSES, jnp.int32),
        'w_stem': normal(2, (PATCH_DIM, CHANNELS), PATCH_DIM ** -0.5),
        'b_stem': normal(3, (CHANNELS,), 0.5),
        'ln1_g': 1.0 + normal(4, chan_shape, 0.3),
        'ln1_b': normal(5, chan_shape, 0.3),
        'w_tok1': normal(6, (LAYERS, TOKENS, TOKEN_HIDDEN), TOKENS ** -0.5),
        'b_tok1': normal(7, (LAYERS, TOKEN_HIDDEN), 0.3),
        'w_tok2': normal(8, (LAYERS, TOKEN_HIDDEN, TOKENS), TOKEN_HIDDEN ** -0.5),
        'ln2_g': 1.0 + normal(9, chan_shape, 0.3),
        'ln2_b': normal(10, chan_shape, 0.3),
        'w_ch1': normal(11, (LAYERS, CHANNELS, CHANNEL_HIDDEN), CHANNELS ** -0.5),
        'b_ch1': normal(12, (LAYERS, CHANNEL_HIDDEN), 0.3),
        'w_ch2': normal(13, (LAYERS, CHANNEL_HIDDEN, CHANNELS), CHANNEL_HIDDEN ** -0.5),
        'b_ch2': normal(14, chan_shape, 0.3),
        'lnf_g': 1.0 + normal(15, (CHANNELS,), 0.3),
        'lnf_b': normal(16, (CHANNELS,), 0.3),
        'w_head': normal(17, (CHANNELS, CLASSES), CHANNELS ** -0.5),
        'b_head': normal(18, (CLASSES,), 0.5),
    }


def as_matmul(values):
    return values.astype(jnp.bfloat16).astype(jnp.float32)


def layer_norm(values, gain, shift):
    mean_val = jnp.mean(values, axis=-1, keepdims=True)
    centered = values - mean_val
    var_val = jnp.mean(centered * centered, axis=-1, keepdims=True)
    return centered * lax.rsqrt(var_val + EPS) * gain + shift


def mixer_layer(resid, layer):
    normed = as_matmul(layer_norm(resid, layer['ln1_g'], layer['ln1_b']))
    hidden = jnp.einsum('bsc,sj->bcj', normed, as_matmul(layer['w_tok1'])) + layer['b_tok1']
    mixed = jnp.einsum('bcj,js->bsc', as_matmul(jax.nn.gelu(hidden)), as_matmul(layer['w_tok2']))
    resid = resid + mixed
    normed = as_matmul(layer_norm(resid, layer['ln2_g'], layer['ln2_b']))
    hidden = jnp.einsum('bsc,cd->bsd', normed, as_matmul(layer['w_ch1'])) + layer['b_ch1']
    out_val = jnp.einsum('bsd,dc->bsc', as_matmul(jax.nn.gelu(hidden)), as_matmul(layer['w_ch2']))
    return resid + out_val + layer['b_ch2'], None


def block_loss(weights, patch_blk, label_blk):
    resid = jnp.einsum('bsp,pc->bsc', patch_blk.astype(jnp.float32), as_matmul(weights['w_stem'])) + weights['b_stem']
    layer_weights = {name: weights[name] for name in LAYER_NAMES}
    resid = lax.scan(mixer_layer, resid, layer_weights)[0]
    pooled = jnp.mean(resid, axis=1)
    normed = as_matmul(layer_norm(pooled, weights['lnf_g'], weights['lnf_b']))
    logits = jnp.einsum('bc,ck->bk', normed, as_matmul(weights['w_head'])) + weights['b_head']
    log_norm = jax.nn.logsumexp(logits, axis=-1)
    class_ids = jnp.arange(CLASSES, dtype=jnp.int32)
    picked = jnp.sum(jnp.where(class_ids[None, :] == label_blk[:, None], logits, 0.0), axis=-1)
    return jnp.sum(log_norm - picked)


def reference(patches, labels, w_stem, b_stem, ln1_g, ln1_b, w_tok1, b_tok1, w_tok2,
              ln2_g, ln2_b, w_ch1, b_ch1, w_ch2, b_ch2, lnf_g, lnf_b, w_head, b_head):
    weights = dict(w_stem=w_stem, b_stem=b_stem, ln1_g=ln1_g, ln1_b=ln1_b, w_tok1=w_tok1,
                   b_tok1=b_tok1, w_tok2=w_tok2, ln2_g=ln2_g, ln2_b=ln2_b, w_ch1=w_ch1,
                   b_ch1=b_ch1, w_ch2=w_ch2, b_ch2=b_ch2, lnf_g=lnf_g, lnf_b=lnf_b,
                   w_head=w_head, b_head=b_head)
    patch_blocks = patches.reshape(BLOCKS, PER_BLOCK, TOKENS, PATCH_DIM)
    label_blocks = labels.reshape(BLOCKS, PER_BLOCK)
    loss_grad = jax.value_and_grad(block_loss)

    def accumulate(carry, block):
        loss_sum, grad_sum = carry
        value, grads = loss_grad(weights, block[0], block[1])
        return (loss_sum + value, jax.tree.map(jnp.add, grad_sum, grads)), None

    start_carry = (jnp.zeros((), jnp.float32), jax.tree.map(jnp.zeros_like, weights))
    loss_sum, grad_sum = lax.scan(accumulate, start_carry, (patch_blocks, label_blocks))[0]
    scale = 1.0 / IMAGES
    return (loss_sum * scale, grad_sum['w_stem'] * scale, grad_sum['b_stem'] * scale,
            grad_sum['ln1_g'] * scale, grad_sum['ln1_b'] * scale, grad_sum['w_tok1'] * scale,
            grad_sum['b_tok1'] * scale, grad_sum['w_tok2'] * scale, grad_sum['ln2_g'] * scale,
            grad_sum['ln2_b'] * scale, grad_sum['w_ch1'] * scale, grad_sum['b_ch1'] * scale,
            grad_sum['w_ch2'] * scale, grad_sum['b_ch2'] * scale, grad_sum['lnf_g'] * scale,
            grad_sum['lnf_b'] * scale, grad_sum['w_head'] * scale, grad_sum['b_head'] * scale)
```

```python
import functools

import jax
import jax.numpy as jnp
from jax import lax
from jax.experimental import pallas as pl
from jax.experimental.pallas import tpu as pltpu
from jax.sharding import PartitionSpec as P

EPS = 1e-6
CHANNEL_AXES = ('tp', 'fsdp')
BF = jnp.bfloat16
F32 = jnp.float32
ORDERS = (('x', 'y', 'z'), ('y', 'z', 'x'), ('z', 'x', 'y'))
BIT = {'x': 0, 'y': 1, 'z': 2}


def product(form, left, right):
    return jnp.einsum(form, left, right, preferred_element_type=F32)


def exchange(values, axis):
    if axis == 'z':
        return lax.ppermute(values, 'tp', [(0, 1), (1, 0)])
    flip = {'core': 1, 'x': 2, 'y': 4}[axis]
    return lax.ppermute(values, 'fsdp', [(i, i ^ flip) for i in range(8)])


def coords():
    f = lax.axis_index('fsdp')
    return lax.axis_index('tp'), f // 4, (f // 2) % 2, f % 2


def chip_gather(part, order):
    b0 = part[None]
    b1 = jnp.concatenate([b0, exchange(b0, order[0])])
    b2 = jnp.concatenate([b1, exchange(b1, order[1])])
    both = [b2, exchange(b2, order[2])]
    return both + [exchange(v, 'core') for v in both]


def source_coords(order, which, entry):
    flips = {'x': 0, 'y': 0, 'z': 0, 'core': which >> 1}
    flips[order[0]] = entry & 1
    flips[order[1]] = entry >> 1
    flips[order[2]] = which & 1
    z, y, x, c = coords()
    flip = lambda v, k: (1 - v) if k else v
    return flip(z, flips['z']), (flip(y, flips['y']) * 2 + flip(x, flips['x'])) * 2 + flip(c, flips['core'])


def assemble_kernel(windows, n_arr, n_out, *refs):
    ins, outs = refs[:n_arr], refs[n_arr:n_arr + n_out]
    bufs = refs[n_arr + n_out:2 * n_arr + n_out]
    sem_in, sem_out = refs[2 * n_arr + n_out:]
    for a in range(n_arr):
        pltpu.make_async_copy(ins[a], bufs[a], sem_in.at[a]).start()
    for a in range(n_arr):
        pltpu.make_async_copy(ins[a], bufs[a], sem_in.at[a]).wait()
        part, which = divmod(a, 4)
        for entry in range(4):
            z, f = source_coords(ORDERS[part], which, entry)
            for (row, rows, out, place) in windows[part]:
                r0, c0, cols = place(z, f)
                pltpu.make_async_copy(
                    bufs[a].at[entry, pl.ds(row, rows), :],
                    outs[out].at[pl.ds(pl.multiple_of(r0, 16), rows), pl.ds(pl.multiple_of(c0, 128), cols)],
                    sem_out.at[a]).start()
    for a in range(n_arr):
        pltpu.make_async_copy(ins[a], bufs[a], sem_out.at[a]).wait()


def assemble(arrays, windows, out_shapes, name):
    n_arr = len(arrays)
    total = sum(v.size for v in arrays) * 2
    return pl.pallas_call(
        functools.partial(assemble_kernel, windows, n_arr, len(out_shapes)),
        out_shape=[jax.ShapeDtypeStruct(s, BF) for s in out_shapes],
        in_specs=[pl.BlockSpec(memory_space=pl.ANY)] * n_arr,
        out_specs=[pl.BlockSpec(memory_space=pl.ANY)] * len(out_shapes),
        scratch_shapes=[pltpu.VMEM(v.shape, BF) for v in arrays] + [pltpu.SemaphoreType.DMA((n_arr,)),
                                                                   pltpu.SemaphoreType.DMA((n_arr,))],
        compiler_params=pltpu.CompilerParams(vmem_limit_bytes=total + (4 << 20)),
        cost_estimate=pl.CostEstimate(flops=8_000_000_000, bytes_accessed=2 * total, transcendentals=0),
        name=name)(*arrays)


def split_rows(total, align):
    first = (total // 3 + align - 1) // align * align
    return [(0, first), (first, first), (2 * first, total - 2 * first)]


def gather_stem(w_piece):
    rows, cols = w_piece.shape
    parts, windows = [], []
    for p, (r0, n) in enumerate(split_rows(rows, 16)):
        parts += chip_gather(lax.slice_in_dim(w_piece, r0, r0 + n), ORDERS[p])
        windows.append([(0, n, 0, lambda z, f, r0=r0: (f * rows + r0, z * cols, cols))])
    return assemble(parts, windows, [(8 * rows, 2 * cols)], 'put_stem')[0]


def gather_layer(w1, w2):
    rows1, cols1 = w1.shape
    rows2, cols2 = w2.shape
    half = cols1 // 2
    parts, windows = [], []
    for p, ((r0, n), (q0, m)) in enumerate(zip(split_rows(rows1, 16), split_rows(rows2, 16))):
        piece = jnp.concatenate([w1[r0:r0 + n, :half], w1[r0:r0 + n, half:], w2[q0:q0 + m]])
        parts += chip_gather(piece, ORDERS[p])
        windows.append([
            (0, n, 0, lambda z, f, r0=r0: (f * rows1 + r0, z * cols1, half)),
            (n, n, 0, lambda z, f, r0=r0: (f * rows1 + r0, z * cols1 + half, half)),
            (2 * n, m, 1, lambda z, f, q0=q0: (z * 8 * rows2 + f * rows2 + q0, 0, cols2))])
    return assemble(parts, windows, [(8 * rows1, 2 * cols1), (16 * rows2, cols2)], 'put_layer')


def send_block(bit, r):
    if bit == 0:
        return jnp.maximum(0, (r + 1) // 2 - 1)
    if bit == 1:
        return jnp.maximum(0, (r // 4) * 2 + jnp.maximum(r % 4 - 2, -1))
    return jnp.maximum(0, r - 4)


def keep_block(bit, r):
    if bit == 0:
        return r // 2
    if bit == 1:
        return (r // 4) * 2 + jnp.minimum(r % 4, 1)
    return jnp.minimum(r, 3)


def wgrad_kernel(splits, place_ref, lo, ls, ro, rs, *outs):
    r = pl.program_id(0)
    dims = (((0,), (0,)), ((), ()))
    tile = lax.dot_general(lo[...], ro[...], dims, preferred_element_type=F32)
    tile += lax.dot_general(ls[...], rs[...], dims, preferred_element_type=F32)
    for p, (r0, n) in enumerate(splits):
        mine = (r >> BIT[ORDERS[p][0]]) & 1
        send, keep = outs[2 * p], outs[2 * p + 1]

        @pl.when(mine == 1)
        def _():
            send[0] = tile[r0:r0 + n]

        @pl.when(mine == 0)
        def _():
            keep[0] = tile[r0:r0 + n]


def weight_grad(left, left_sib, right, right_sib, rows, cols, left_by_z, name):
    k = left.shape[0]
    z, y, x, c = coords()
    place = jnp.stack([z, y, x, c]).astype(jnp.int32)
    splits = split_rows(rows, 8)

    def left_map(r, s):
        f = ((s[1] ^ ((r >> 1) & 1)) * 2 + (s[2] ^ (r & 1))) * 2 + s[3]
        return (0, (s[0] ^ (r >> 2)) * 8 + f) if left_by_z else (0, f)

    def right_map(r, s):
        return (0, 0) if left_by_z else (0, s[0] ^ (r >> 2))

    out_shape, out_specs = [], []
    for p, (_, n) in enumerate(splits):
        bit = BIT[ORDERS[p][0]]
        for block in (send_block, keep_block):
            out_shape.append(jax.ShapeDtypeStruct((4, n, cols), F32))
            out_specs.append(pl.BlockSpec((1, n, cols), lambda r, s, block=block, bit=bit: (block(bit, r), 0, 0)))
    outs = pl.pallas_call(
        functools.partial(wgrad_kernel, splits),
        out_shape=out_shape,
        grid_spec=pltpu.PrefetchScalarGridSpec(
            num_scalar_prefetch=1, grid=(8,),
            in_specs=[pl.BlockSpec((k, rows), left_map)] * 2 + [pl.BlockSpec((k, cols), right_map)] * 2,
            out_specs=out_specs),
        compiler_params=pltpu.CompilerParams(vmem_limit_bytes=48 << 20),
        cost_estimate=pl.CostEstimate(flops=2 * 2 * k * rows * cols * 8, bytes_accessed=40_000_000, transcendentals=0),
        name=name)(place, left, left_sib, right, right_sib)
    done = []
    for p in range(3):
        a1, a2, a3 = ORDERS[p]
        send, keep = outs[2 * p], outs[2 * p + 1]
        got = exchange(send, a1)
        others = sorted([BIT[a2], BIT[a3]])
        high = BIT[a2] == others[1]
        pick = (lambda v, k: v[2 * k:2 * k + 2]) if high else (lambda v, k: v[k::2])
        send = pick(keep, 1) + pick(got, 1)
        keep = pick(keep, 0) + pick(got, 0)
        got = exchange(send, a2)
        send = keep[1] + got[1]
        keep = keep[0] + got[0]
        done.append(keep + exchange(send, a3))
    return jnp.concatenate(done)


def norm_forward(values, gain, shift):
    width = values.shape[-1]
    mean_val = jnp.sum(values, axis=-1, keepdims=True) / width
    centered = values - mean_val
    var_val = jnp.sum(centered * centered, axis=-1, keepdims=True) / width
    inv_std = lax.rsqrt(var_val + EPS)
    standard = centered * inv_std
    return standard * gain + shift, standard, inv_std


def norm_backward(grad_out, gain, standard, inv_std):
    width = grad_out.shape[-1]
    grad_std = grad_out * gain
    m0 = jnp.sum(grad_std, axis=-1, keepdims=True) / width
    m1 = jnp.sum(grad_std * standard, axis=-1, keepdims=True) / width
    return inv_std * (grad_std - m0 - standard * m1)


def gelu_grad(pre_act, grad_out):
    return jax.vjp(jax.nn.gelu, pre_act)[1](grad_out)[0]


def weight_specs():
    vec_spec = P(CHANNEL_AXES)
    layer_vec = P(None, CHANNEL_AXES)
    return (P('fsdp', 'tp'), vec_spec, layer_vec, layer_vec, P(None, None, 'fsdp'), P(None, 'fsdp'),
            P(None, 'fsdp', None), layer_vec, layer_vec, P(None, 'fsdp', 'tp'), layer_vec,
            P(None, CHANNEL_AXES, None), layer_vec, vec_spec, vec_spec, P('fsdp', 'tp'), P('tp'))


def lead_sum(values):
    return jnp.sum(values, axis=tuple(range(values.ndim - 1)))


def solution(mesh):
    fsdp_size = mesh.shape['fsdp']
    tp_size = mesh.shape['tp']

    def step(patches, labels, w_stem, b_stem, ln1_g, ln1_b, w_tok1, b_tok1, w_tok2,
             ln2_g, ln2_b, w_ch1, b_ch1, w_ch2, b_ch2, lnf_g, lnf_b, w_head, b_head):
        layers = w_tok1.shape[0]
        images = patches.shape[0] // tp_size
        tokens = patches.shape[1]
        channels = w_stem.shape[1] * tp_size
        hidden = w_ch1.shape[2] * tp_size
        tok_hidden = w_tok1.shape[2] * fsdp_size
        classes = w_head.shape[1] * tp_size
        total_images = images * tp_size * fsdp_size
        rows = images * tokens
        z_idx, f_idx = lax.axis_index('tp'), lax.axis_index('fsdp')

        stem_full = gather_stem(w_stem.astype(BF))
        layer_full = [gather_layer(w_ch1[i].astype(BF), w_ch2[i].astype(BF)) for i in range(layers)]

        mine = lax.dynamic_slice_in_dim(patches, z_idx * images, images, 0)
        mine = jnp.transpose(mine, (1, 0, 2)).reshape(rows, -1)
        mine_sib = exchange(mine, 'core')
        my_labels = lax.dynamic_slice_in_dim(labels, z_idx * images, images, 0)

        packed_names = [b_stem, ln1_g, ln1_b, ln2_g, ln2_b, b_ch1, b_ch2, lnf_g, lnf_b]
        small = [v.reshape(-1) for v in packed_names + [b_tok1, w_tok1, w_tok2, b_head]]
        sizes = [v.shape[0] for v in small]
        full_small = lax.all_gather(jnp.concatenate(small), ('tp', 'fsdp'), axis=0)
        pieces, at = [], 0
        for n in sizes:
            pieces.append(full_small[:, at:at + n])
            at += n

        def vec(i):
            return pieces[i].reshape(-1)

        def layer_vec(i):
            return jnp.transpose(pieces[i].reshape(16, layers, -1), (1, 0, 2)).reshape(layers, -1)

        stem_bias = vec(0)
        ln1_gain, ln1_shift, ln2_gain, ln2_shift, ch_bias1, ch_bias2 = [layer_vec(i) for i in range(1, 7)]
        lnf_gain, lnf_shift = vec(7), vec(8)
        tok_bias = jnp.transpose(pieces[9][:8].reshape(8, layers, -1), (1, 0, 2)).reshape(layers, -1)
        tok_w1 = jnp.transpose(pieces[10][:8].reshape(8, layers, tokens, -1), (1, 2, 0, 3)).reshape(
            layers, tokens, tok_hidden).astype(BF)
        tok_w2 = jnp.transpose(pieces[11][:8].reshape(8, layers, -1, tokens), (1, 0, 2, 3)).reshape(
            layers, tok_hidden, tokens).astype(BF)
        head_bias = jnp.stack([pieces[12][0], pieces[12][8]]).reshape(classes)

        head_own = lax.all_gather(w_head.astype(BF), 'fsdp', axis=0, tiled=True)
        head_other = exchange(head_own, 'z')
        head_w = jnp.where(z_idx == 0, jnp.concatenate([head_own, head_other], axis=1),
                           jnp.concatenate([head_other, head_own], axis=1))

        resid = (product('rp,pc->rc', mine, stem_full) + stem_bias).reshape(tokens, images, channels)
        saved = []
        for layer in range(layers):
            ch_w1, ch_w2 = layer_full[layer]
            normed, norm1_std, norm1_inv = norm_forward(resid, ln1_gain[layer], ln1_shift[layer])
            normed = normed.astype(BF)
            tok_pre = product('sbc,sj->bcj', normed, tok_w1[layer]) + tok_bias[layer]
            tok_act = jax.nn.gelu(tok_pre).astype(BF)
            resid = resid + product('bcj,js->sbc', tok_act, tok_w2[layer])
            normed2, norm2_std, norm2_inv = norm_forward(resid, ln2_gain[layer], ln2_shift[layer])
            full_in = normed2.astype(BF).reshape(rows, channels)
            ch_pre = product('rc,cd->rd', full_in, ch_w1) + ch_bias1[layer]
            ch_act = jax.nn.gelu(ch_pre).astype(BF)
            out = product('rd,dc->rc', ch_act, ch_w2).reshape(tokens, images, channels)
            resid = resid + out + ch_bias2[layer]
            saved.append(dict(normed=normed, norm1_std=norm1_std, norm1_inv=norm1_inv, tok_pre=tok_pre,
                              tok_act=tok_act, norm2_std=norm2_std, norm2_inv=norm2_inv,
                              full_in=full_in, ch_pre=ch_pre, ch_act=ch_act,
                              full_in_sib=exchange(full_in, 'core'), ch_act_sib=exchange(ch_act, 'core')))

        pooled = jnp.mean(resid, axis=0)
        head_in, head_std, head_inv = norm_forward(pooled, lnf_gain, lnf_shift)
        head_in = head_in.astype(BF)
        logits = product('bc,ck->bk', head_in, head_w) + head_bias
        is_label = jnp.arange(classes)[None, :] == my_labels[:, None]
        row_max = jnp.max(logits, axis=1, keepdims=True)
        shifted = jnp.exp(logits - row_max)
        class_sum = jnp.sum(shifted, axis=1, keepdims=True)
        log_norm = row_max + jnp.log(class_sum)
        loss_part = jnp.sum(log_norm[:, 0] - jnp.sum(jnp.where(is_label, logits, 0.0), axis=1)) / total_images
        d_logits = (shifted / class_sum - is_label.astype(F32)) / total_images
        d_logits_bf = d_logits.astype(BF)
        g_b_head_part = jnp.sum(d_logits, axis=0)

        pad = jnp.zeros((images, 1024 - classes), BF)
        both = lax.all_gather(jnp.concatenate([head_in, d_logits_bf, pad], axis=1), ('tp', 'fsdp'), axis=0, tiled=True)
        head_rows = w_head.shape[0]
        half = classes // tp_size
        d_cols = jnp.where(z_idx == 0, both[:, channels:channels + half], both[:, channels + half:channels + classes])
        g_w_head = product('bc,bk->ck', lax.dynamic_slice_in_dim(both, f_idx * head_rows, head_rows, 1), d_cols)

        d_head_in = product('bk,ck->bc', d_logits_bf, head_w)
        g_lnf_g = jnp.sum(d_head_in * head_std, axis=0)
        g_lnf_b = jnp.sum(d_head_in, axis=0)
        d_pooled = norm_backward(d_head_in, lnf_gain, head_std, head_inv)
        d_resid = jnp.broadcast_to((d_pooled / tokens)[None], (tokens, images, channels))

        big = {name: [None] * layers for name in ('w_ch1', 'w_ch2')}
        little = {}
        for layer in reversed(range(layers)):
            keep = saved[layer]
            ch_w1, ch_w2 = layer_full[layer]
            little['b_ch2', layer] = lead_sum(d_resid)
            d_out = d_resid.astype(BF).reshape(rows, channels)
            d_out_sib = exchange(d_out, 'core')
            big['w_ch2'][layer] = weight_grad(keep['ch_act'], keep['ch_act_sib'], d_out, d_out_sib,
                                              w_ch2.shape[1], channels, True, 'grad_ch2')
            d_ch_pre = gelu_grad(keep['ch_pre'], product('rc,dc->rd', d_out, ch_w2))
            little['b_ch1', layer] = lead_sum(d_ch_pre)
            d_ch_pre = d_ch_pre.astype(BF)
            d_ch_pre_sib = exchange(d_ch_pre, 'core')
            big['w_ch1'][layer] = weight_grad(keep['full_in'], keep['full_in_sib'], d_ch_pre, d_ch_pre_sib,
                                              w_ch1.shape[1], w_ch1.shape[2], False, 'grad_ch1')
            d_norm2 = product('rd,cd->rc', d_ch_pre, ch_w1).reshape(tokens, images, channels)
            little['ln2_g', layer] = lead_sum(d_norm2 * keep['norm2_std'])
            little['ln2_b', layer] = lead_sum(d_norm2)
            d_mid = d_resid + norm_backward(d_norm2, ln2_gain[layer], keep['norm2_std'], keep['norm2_inv'])
            d_mid_bf = d_mid.astype(BF)
            little['w_tok2', layer] = product('bcj,sbc->js', keep['tok_act'], d_mid_bf)
            d_tok_pre = gelu_grad(keep['tok_pre'], product('sbc,js->bcj', d_mid_bf, tok_w2[layer]))
            little['b_tok1', layer] = lead_sum(d_tok_pre)
            d_tok_pre = d_tok_pre.astype(BF)
            little['w_tok1', layer] = product('sbc,bcj->sj', keep['normed'], d_tok_pre)
            d_norm1 = product('bcj,sj->sbc', d_tok_pre, tok_w1[layer])
            little['ln1_g', layer] = lead_sum(d_norm1 * keep['norm1_std'])
            little['ln1_b', layer] = lead_sum(d_norm1)
            d_resid = d_mid + norm_backward(d_norm1, ln1_gain[layer], keep['norm1_std'], keep['norm1_inv'])

        little['b_stem', 0] = lead_sum(d_resid)
        d_stem = d_resid.astype(BF).reshape(rows, channels)
        g_w_stem = weight_grad(mine, mine_sib, d_stem, exchange(d_stem, 'core'),
                               w_stem.shape[0], w_stem.shape[1], False, 'grad_stem')

        little['lnf_g', 0], little['lnf_b', 0], little['b_head', 0] = g_lnf_g, g_lnf_b, g_b_head_part
        little['loss', 0] = loss_part[None]
        keys = list(little)
        summed = lax.psum(jnp.concatenate([little[k].reshape(-1) for k in keys]), ('tp', 'fsdp'))
        total, at = {}, 0
        for k in keys:
            total[k] = summed[at:at + little[k].size].reshape(little[k].shape)
            at += little[k].size

        def own(value, axis, by_tp=True):
            n = value.shape[axis] // (fsdp_size * (tp_size if by_tp else 1))
            return lax.dynamic_slice_in_dim(value, (f_idx + (z_idx * fsdp_size if by_tp else 0)) * n, n, axis)

        def per_layer(name, axis, by_tp=True):
            return own(jnp.stack([total[name, i] for i in range(layers)]), axis + 1, by_tp)

        return (total['loss', 0][0], g_w_stem, own(total['b_stem', 0], 0), per_layer('ln1_g', 0),
                per_layer('ln1_b', 0), per_layer('w_tok1', 1, False), per_layer('b_tok1', 0, False),
                per_layer('w_tok2', 0, False), per_layer('ln2_g', 0), per_layer('ln2_b', 0),
                jnp.stack(big['w_ch1']), per_layer('b_ch1', 0), jnp.stack(big['w_ch2']), per_layer('b_ch2', 0),
                own(total['lnf_g', 0], 0), own(total['lnf_b', 0], 0), g_w_head,
                lax.dynamic_slice_in_dim(total['b_head', 0], z_idx * half, half, 0))

    specs = weight_specs()
    return jax.shard_map(step, mesh=mesh, in_specs=(P('fsdp', None, None), P('fsdp')) + specs,
                         out_specs=(P(),) + specs, check_vma=False)
```

```python
import functools

import jax
import jax.numpy as jnp
from jax import lax
from jax.experimental import pallas as pl
from jax.experimental.pallas import tpu as pltpu
from jax.sharding import PartitionSpec as P

EPS = 1e-6
CHANNEL_AXES = ('tp', 'fsdp')
BF = jnp.bfloat16
F32 = jnp.float32
ORDERS = (('x', 'y', 'z'), ('y', 'z', 'x'), ('z', 'x', 'y'))
BIT = {'x': 0, 'y': 1, 'z': 2}


def product(form, left, right):
    return jnp.einsum(form, left, right, preferred_element_type=F32)


def exchange(values, axis):
    if axis == 'z':
        return lax.ppermute(values, 'tp', [(0, 1), (1, 0)])
    flip = {'core': 1, 'x': 2, 'y': 4}[axis]
    return lax.ppermute(values, 'fsdp', [(i, i ^ flip) for i in range(8)])


def coords():
    f = lax.axis_index('fsdp')
    return lax.axis_index('tp'), f // 4, (f // 2) % 2, f % 2


class Gathering:
    def __init__(self, parts):
        self.held, self.stage, self.got = [p[None] for p in parts], 0, None

    def arrived(self):
        return self.got or []

    def receive(self, values):
        self.got = list(values)

    def pending(self):
        return self.held

    def replace(self, values):
        self.held = list(values)

    def launch(self):
        self.got = [exchange(v, ORDERS[p][self.stage]) for p, v in enumerate(self.held)]
        self.stage += 1

    def fold(self):
        self.held = [jnp.concatenate([v, g]) for v, g in zip(self.held, self.got)]

    def finish(self, after=None):
        arrays = []
        if after is not None:
            self.got = list(lax.optimization_barrier((after, *self.got))[1:])
        for v, g in zip(self.held, self.got):
            arrays += [v, g, exchange(v, 'core'), exchange(g, 'core')]
        return arrays


class Doubling:
    AXES = ('core', 'x', 'y', 'z')

    def __init__(self, value, gather):
        self.value, self.gather, self.stage, self.got = value, gather, 0, None

    def arrived(self):
        return [] if self.got is None else [self.got]

    def receive(self, values):
        self.got = values[0]

    def pending(self):
        return [self.value]

    def replace(self, values):
        self.value = values[0]

    def launch(self):
        self.got = exchange(self.value, self.AXES[self.stage])
        self.stage += 1

    def fold(self):
        self.value = jnp.concatenate([self.value, self.got]) if self.gather else self.value + self.got


def fence(value, *transfers):
    flat = [v for t in transfers for v in t.arrived()]
    if flat:
        out = lax.optimization_barrier((value, *flat))
        value, at = out[0], 1
        for t in transfers:
            n = len(t.arrived())
            if n:
                t.receive(out[at:at + n])
                at += n
                t.fold()
    flat = [v for t in transfers for v in t.pending()]
    out = lax.optimization_barrier((value, *flat))
    at = 1
    for t in transfers:
        n = len(t.pending())
        t.replace(out[at:at + n])
        at += n
        t.launch()
    return out[0]


def gate(value, other):
    return lax.optimization_barrier((value, other))[0]


def merge_absolute(value, axis):
    bit, dim = {'z': (0, 0), 'y': (1, 1), 'x': (2, 2), 'core': (3, 3)}[axis]
    other = exchange(value, axis)
    low = jnp.where(coords()[bit] == 0, value, other)
    high = jnp.where(coords()[bit] == 0, other, value)
    return jnp.concatenate([low, high], axis=dim)


def source_coords(order, which, entry):
    flips = {'x': 0, 'y': 0, 'z': 0, 'core': which >> 1}
    flips[order[0]] = entry & 1
    flips[order[1]] = entry >> 1
    flips[order[2]] = which & 1
    z, y, x, c = coords()
    flip = lambda v, k: (1 - v) if k else v
    return flip(z, flips['z']), (flip(y, flips['y']) * 2 + flip(x, flips['x'])) * 2 + flip(c, flips['core'])


def assemble_kernel(windows, n_arr, n_out, *refs):
    ins, outs = refs[:n_arr], refs[n_arr:n_arr + n_out]
    bufs = refs[n_arr + n_out:2 * n_arr + n_out]
    sem_in, sem_out = refs[2 * n_arr + n_out:]
    for a in range(n_arr):
        pltpu.make_async_copy(ins[a], bufs[a], sem_in.at[a]).start()
    for a in range(n_arr):
        pltpu.make_async_copy(ins[a], bufs[a], sem_in.at[a]).wait()
        part, which = divmod(a, 4)
        for entry in range(4):
            z, f = source_coords(ORDERS[part], which, entry)
            for (row, rows, col, out, place) in windows[part]:
                r0, c0, cols = place(z, f)
                pltpu.make_async_copy(
                    bufs[a].at[entry, pl.ds(row, rows), pl.ds(col, cols)],
                    outs[out].at[pl.ds(pl.multiple_of(r0, 16), rows), pl.ds(pl.multiple_of(c0, 128), cols)],
                    sem_out.at[a]).start()
    for a in range(n_arr):
        pltpu.make_async_copy(ins[a], bufs[a], sem_out.at[a]).wait()


def assemble(arrays, windows, out_shapes, name):
    n_arr = len(arrays)
    total = sum(v.size for v in arrays) * 2
    return pl.pallas_call(
        functools.partial(assemble_kernel, windows, n_arr, len(out_shapes)),
        out_shape=[jax.ShapeDtypeStruct(s, BF) for s in out_shapes],
        in_specs=[pl.BlockSpec(memory_space=pl.ANY)] * n_arr,
        out_specs=[pl.BlockSpec(memory_space=pl.ANY)] * len(out_shapes),
        scratch_shapes=[pltpu.VMEM(v.shape, BF) for v in arrays] + [pltpu.SemaphoreType.DMA((n_arr,)),
                                                                   pltpu.SemaphoreType.DMA((n_arr,))],
        compiler_params=pltpu.CompilerParams(vmem_limit_bytes=total + (4 << 20)),
        cost_estimate=pl.CostEstimate(flops=8_000_000_000, bytes_accessed=2 * total, transcendentals=0),
        name=name)(*arrays)


def split_rows(total, align):
    first = (total // 3 + align - 1) // align * align
    return [(0, first), (first, first), (2 * first, total - 2 * first)]


def stem_pieces(w_piece):
    rows, cols = w_piece.shape
    parts, windows = [], []
    for r0, n in split_rows(rows, 16):
        parts.append(lax.slice_in_dim(w_piece, r0, r0 + n))
        windows.append([(0, n, 0, 0, lambda z, f, r0=r0: (f * rows + r0, z * cols, cols))])
    return Gathering(parts), windows


def layer_pieces(w1, w2, head=None):
    rows1, cols1 = w1.shape
    rows2, cols2 = w2.shape
    half = cols1 // 2
    parts, windows = [], []
    splits = [split_rows(rows1, 16), split_rows(rows2, 16), [(0, 16), (16, 16), (32, 32)]]
    for (r0, n), (q0, m), (h0, k) in zip(*splits):
        piece = [w1[r0:r0 + n, :half], w1[r0:r0 + n, half:], w2[q0:q0 + m]]
        window = [
            (0, n, 0, 0, lambda z, f, r0=r0: (f * rows1 + r0, z * cols1, half)),
            (n, n, 0, 0, lambda z, f, r0=r0: (f * rows1 + r0, z * cols1 + half, half)),
            (2 * n, m, 0, 1, lambda z, f, q0=q0: (z * 8 * rows2 + f * rows2 + q0, 0, cols2))]
        if head is not None:
            wide = head.shape[1]
            piece.append(jnp.concatenate([head[h0:h0 + k], head[64 + h0:64 + h0 + k]], axis=1))
            window += [(2 * n + m, k, 0, 2, lambda z, f, h0=h0: (f * 128 + h0, z * wide, wide)),
                       (2 * n + m, k, wide, 2, lambda z, f, h0=h0: (f * 128 + 64 + h0, z * wide, wide))]
        parts.append(jnp.concatenate(piece))
        windows.append(window)
    return Gathering(parts), windows


def send_block(bit, r):
    if bit == 0:
        return jnp.maximum(0, (r + 1) // 2 - 1)
    if bit == 1:
        return jnp.maximum(0, (r // 4) * 2 + jnp.maximum(r % 4 - 2, -1))
    return jnp.maximum(0, r - 4)


def keep_block(bit, r):
    if bit == 0:
        return r // 2
    if bit == 1:
        return (r // 4) * 2 + jnp.minimum(r % 4, 1)
    return jnp.minimum(r, 3)


def store_parts(outs, at, tile, splits, r):
    for p, (r0, n) in enumerate(splits):
        mine = (r >> BIT[ORDERS[p][0]]) & 1
        send, keep = outs[2 * p], outs[2 * p + 1]

        @pl.when(mine == 1)
        def _():
            send[0, at[p]:at[p] + n] = tile[r0:r0 + n]

        @pl.when(mine == 0)
        def _():
            keep[0, at[p]:at[p] + n] = tile[r0:r0 + n]


def grad_tile(lo, ls, ro, rs):
    dims = (((0,), (0,)), ((), ()))
    return (lax.dot_general(lo, ro, dims, preferred_element_type=F32)
            + lax.dot_general(ls, rs, dims, preferred_element_type=F32))


def stem_grad_kernel(splits, place_ref, lo, ls, ro, rs, *outs):
    store_parts(outs, (0, 0, 0), grad_tile(lo[...], ls[...], ro[...], rs[...]), splits, pl.program_id(0))


def layer_grad_kernel(splits1, splits2, place_ref, lo2, ls2, ro2, rs2, lo1, ls1, ro1, rs1, *outs):
    r = pl.program_id(0)
    half = ro1.shape[1] // 2
    for k in range(2):
        cols = slice(k * half, (k + 1) * half)
        at = [k * n for _, n in splits1]
        store_parts(outs, at, grad_tile(lo1[...], ls1[...], ro1[:, cols], rs1[:, cols]), splits1, r)
    at = [2 * n for _, n in splits1]
    store_parts(outs, at, grad_tile(lo2[...], ls2[...], ro2[...], rs2[...]), splits2, r)


def file_of(r, s):
    return ((s[1] ^ ((r >> 1) & 1)) * 2 + (s[2] ^ (r & 1))) * 2 + s[3]


def halves_of(r, s):
    return s[0] ^ (r >> 2)


def run_grad(kernel, part_rows, cols, in_specs, operands, flops, name):
    place = jnp.stack(coords()).astype(jnp.int32)
    out_shape, out_specs = [], []
    for p, n in enumerate(part_rows):
        bit = BIT[ORDERS[p][0]]
        for block in (send_block, keep_block):
            out_shape.append(jax.ShapeDtypeStruct((4, n, cols), F32))
            out_specs.append(pl.BlockSpec((1, n, cols), lambda r, s, block=block, bit=bit: (block(bit, r), 0, 0)))
    outs = pl.pallas_call(
        kernel, out_shape=out_shape,
        grid_spec=pltpu.PrefetchScalarGridSpec(num_scalar_prefetch=1, grid=(8,), in_specs=in_specs,
                                               out_specs=out_specs),
        compiler_params=pltpu.CompilerParams(vmem_limit_bytes=56 << 20),
        cost_estimate=pl.CostEstimate(flops=flops, bytes_accessed=40_000_000, transcendentals=0),
        name=name)(place, *operands)
    return Halving(outs)


def stem_grad(left, left_sib, right, right_sib, rows, cols):
    k = left.shape[0]
    splits = split_rows(rows, 8)
    specs = ([pl.BlockSpec((k, rows), lambda r, s: (0, file_of(r, s)))] * 2
             + [pl.BlockSpec((k, cols), lambda r, s: (0, halves_of(r, s)))] * 2)
    return run_grad(functools.partial(stem_grad_kernel, splits), [n for _, n in splits], cols, specs,
                    (left, left_sib, right, right_sib), 32 * k * rows * cols, 'grad_stem')


GRAD_SPLITS1 = [(0, 40), (40, 40), (80, 48)]


def layer_grad(act, act_sib, d_out, d_out_sib, full_in, full_in_sib, d_pre, d_pre_sib, rows1, cols1, rows2, cols2):
    k = act.shape[0]
    splits2 = split_rows(rows2, 8)
    specs = ([pl.BlockSpec((k, rows2), lambda r, s: (0, halves_of(r, s) * 8 + file_of(r, s)))] * 2
             + [pl.BlockSpec((k, cols2), lambda r, s: (0, 0))] * 2
             + [pl.BlockSpec((k, rows1), lambda r, s: (0, file_of(r, s)))] * 2
             + [pl.BlockSpec((k, cols1), lambda r, s: (0, halves_of(r, s)))] * 2)
    part_rows = [2 * n + m for (_, n), (_, m) in zip(GRAD_SPLITS1, splits2)]
    return run_grad(functools.partial(layer_grad_kernel, GRAD_SPLITS1, splits2), part_rows, cols2, specs,
                    (act, act_sib, d_out, d_out_sib, full_in, full_in_sib, d_pre, d_pre_sib),
                    64 * k * rows2 * cols2, 'grad_layer')


class Halving:
    def __init__(self, outs):
        self.send, self.keep, self.stage, self.got = list(outs[0::2]), list(outs[1::2]), 0, None

    def arrived(self):
        return self.got or []

    def receive(self, values):
        self.got = list(values)

    def pending(self):
        return self.send + self.keep

    def replace(self, values):
        n = len(self.send)
        self.send, self.keep = list(values[:n]), list(values[n:])

    def launch(self):
        self.got = [exchange(v, ORDERS[p][self.stage]) for p, v in enumerate(self.send)]
        self.stage += 1

    def fold(self):
        send, keep = [], []
        for p, got in enumerate(self.got):
            old = self.keep[p]
            if self.stage == 1:
                _, a2, a3 = ORDERS[p]
                high = BIT[a2] > BIT[a3]
                pick = (lambda v, k: v[2 * k:2 * k + 2]) if high else (lambda v, k: v[k::2])
                send.append(pick(old, 1) + pick(got, 1))
                keep.append(pick(old, 0) + pick(got, 0))
            else:
                send.append(old[1] + got[1])
                keep.append(old[0] + got[0])
        self.send, self.keep = send, keep

    def close(self, value):
        out = lax.optimization_barrier((value, *self.got))
        self.done = [k + g for k, g in zip(self.keep, out[1:])]
        out = lax.optimization_barrier((out[0], *self.done))
        self.done = list(out[1:])
        return out[0]


def split_layer_grad(parts):
    lo = jnp.concatenate([v[:n] for v, (_, n) in zip(parts, GRAD_SPLITS1)])
    hi = jnp.concatenate([v[n:2 * n] for v, (_, n) in zip(parts, GRAD_SPLITS1)])
    return jnp.concatenate([lo, hi], axis=1), jnp.concatenate([v[2 * n:] for v, (_, n) in zip(parts, GRAD_SPLITS1)])


GELU_A = 0.7978845608028654
GELU_B = 0.044715 * GELU_A
CHUNK = 256
FORWARD_CHUNK = 1024


def row_norm(values):
    mean_val = jnp.mean(values, axis=-1, keepdims=True)
    centered = values - mean_val
    inv_std = lax.rsqrt(jnp.mean(centered * centered, axis=-1, keepdims=True) + EPS)
    return centered * inv_std, inv_std


def row_norm_grad(grad_out, gain, standard, inv_std):
    grad_std = grad_out * gain
    m0 = jnp.mean(grad_std, axis=-1, keepdims=True)
    m1 = jnp.mean(grad_std * standard, axis=-1, keepdims=True)
    return inv_std * (grad_std - m0 - standard * m1)


def dot_dims(left, right, lc, rc):
    return lax.dot_general(left, right, (((lc,), (rc,)), ((), ())), preferred_element_type=F32)


def flip_weight(buf, weight):
    buf[...] = weight[...].astype(F32).T.astype(BF)


def token_forward_kernel(x_ref, g1, s1, g2, s2, w1, bias, w2t, out_ref, v_ref, a_buf, w1t_buf):
    @pl.when(pl.program_id(0) == 0)
    def _():
        flip_weight(w1t_buf, w1)

    x = x_ref[0]
    a_buf[...] = (row_norm(x)[0] * g1[...] + s1[...]).astype(BF)
    for at in range(0, x.shape[1], FORWARD_CHUNK):
        cols = slice(at, at + FORWARD_CHUNK)
        h = dot_dims(w1t_buf[...], a_buf[:, cols], 1, 0) + bias[...]
        t = jnp.tanh(h * (GELU_A + GELU_B * (h * h)))
        act = ((0.5 * h) * (1.0 + t)).astype(BF)
        out_ref[0, :, cols] = x_ref[0, :, cols] + dot_dims(w2t[...], act, 1, 0)
    v_ref[0] = (row_norm(out_ref[0])[0] * g2[...] + s2[...]).astype(BF)


def whole(shape):
    return pl.BlockSpec(shape, lambda i: (0,) * len(shape))


def token_forward(x, g1, s1, g2, s2, w1, bias, w2t):
    images, tokens, channels = x.shape
    hid = w1.shape[1]
    image = pl.BlockSpec((1, tokens, channels), lambda i: (i, 0, 0))
    flops = 4 * images * tokens * channels * hid
    return pl.pallas_call(
        token_forward_kernel, grid=(images,),
        out_shape=[jax.ShapeDtypeStruct(x.shape, F32), jax.ShapeDtypeStruct(x.shape, BF)],
        in_specs=[image] + [whole((1, channels))] * 4 + [whole((tokens, hid)), whole((hid, 1)), whole((tokens, hid))],
        out_specs=[image, image],
        scratch_shapes=[pltpu.VMEM((tokens, channels), BF), pltpu.VMEM((hid, tokens), BF)],
        compiler_params=pltpu.CompilerParams(vmem_limit_bytes=32 << 20),
        cost_estimate=pl.CostEstimate(flops=3 * flops, bytes_accessed=10 * x.size, transcendentals=0),
        name='token_forward')(x, g1, s1, g2, s2, w1, bias, w2t)


def token_backward_kernel(x_ref, mid_ref, dr_ref, dn_ref, g1, s1, g2, w1, bias, w2t, more_ref,
                          dx_ref, dxb_ref, pack_ref, a_buf, dm_buf, da_buf,
                          w1t_buf, w2_buf, acc1, acc2, accb, vec_ref):
    hid = w1.shape[1]
    dn = dn_ref[0]
    std2, inv2 = row_norm(mid_ref[0])
    d_mid = dr_ref[0] + row_norm_grad(dn, g2[...], std2, inv2)
    dm_buf[...] = d_mid.astype(BF)
    std1, inv1 = row_norm(x_ref[0])
    a_buf[...] = (std1 * g1[...] + s1[...]).astype(BF)

    @pl.when(pl.program_id(0) == 0)
    def _():
        vec_ref[...] = jnp.zeros_like(vec_ref)
        acc1[...] = jnp.zeros_like(acc1)
        acc2[...] = jnp.zeros_like(acc2)
        accb[...] = jnp.zeros_like(accb)
        flip_weight(w1t_buf, w1)
        flip_weight(w2_buf, w2t)

    for at in range(0, dn.shape[1], CHUNK):
        cols = slice(at, at + CHUNK)
        a = a_buf[:, cols]
        dm = dm_buf[:, cols]
        h = dot_dims(w1t_buf[...], a, 1, 0) + bias[...]
        sq = h * h
        t = jnp.tanh(h * (GELU_A + GELU_B * sq))
        half_t = 0.5 + 0.5 * t
        act = (h * half_t).astype(BF)
        slope = half_t + (0.5 * h) * (1.0 - t * t) * (GELU_A + (3.0 * GELU_B) * sq)
        d_h = dot_dims(w2_buf[...], dm, 1, 0) * slope
        accb[...] += sum(d_h[:, k:k + 128] for k in range(0, CHUNK, 128))
        d_hb = d_h.astype(BF)
        acc1[...] += dot_dims(d_hb, a, 1, 1)
        acc2[...] += dot_dims(act, dm, 1, 1)
        da_buf[:, cols] = dot_dims(w1[...], d_hb, 1, 0)
    da = da_buf[...]
    dx = d_mid + row_norm_grad(da, g1[...], std1, inv1)
    dx_ref[0] = dx
    dxb_ref[0] = dx.astype(BF)
    for k, v in enumerate((da * std1, da, dn * std2, dn, dx)):
        vec_ref[k:k + 1] += jnp.sum(v, axis=0, keepdims=True)

    @pl.when(pl.program_id(0) == pl.num_programs(0) - 1)
    def _():
        pack_ref[0:8] = vec_ref[...]
        pack_ref[5:6, :hid] = jnp.sum(accb[...].T, axis=0, keepdims=True)
        pack_ref[8:8 + acc1.shape[1], :hid] = acc1[...].T
        pack_ref[8:8 + acc1.shape[1], hid:] = acc2[...].T
        pack_ref[64:] = more_ref[...]


def token_backward(x, mid, dr, dn, g1, s1, g2, w1, bias, w2t, more):
    images, tokens, channels = x.shape
    hid = w1.shape[1]
    image = pl.BlockSpec((1, tokens, channels), lambda i: (i, 0, 0))
    flops = 10 * images * tokens * channels * hid
    return pl.pallas_call(
        token_backward_kernel, grid=(images,),
        out_shape=[jax.ShapeDtypeStruct(x.shape, F32), jax.ShapeDtypeStruct(x.shape, BF),
                   jax.ShapeDtypeStruct((80, channels), F32)],
        in_specs=[image] * 4 + [whole((1, channels))] * 3 + [whole((tokens, hid)), whole((hid, 1)),
                                                            whole((tokens, hid)), whole((16, channels))],
        out_specs=[image, image, whole((80, channels))],
        scratch_shapes=[pltpu.VMEM((tokens, channels), BF), pltpu.VMEM((tokens, channels), BF),
                        pltpu.VMEM((tokens, channels), F32), pltpu.VMEM((hid, tokens), BF),
                        pltpu.VMEM((hid, tokens), BF), pltpu.VMEM((hid, tokens), F32), pltpu.VMEM((hid, tokens), F32),
                        pltpu.VMEM((hid, 128), F32), pltpu.VMEM((8, channels), F32)],
        compiler_params=pltpu.CompilerParams(vmem_limit_bytes=40 << 20),
        cost_estimate=pl.CostEstimate(flops=2 * flops, bytes_accessed=22 * x.size, transcendentals=0),
        name='token_backward')(x, mid, dr, dn, g1, s1, g2, w1, bias, w2t, more)


def norm_forward(values, gain, shift):
    width = values.shape[-1]
    mean_val = jnp.sum(values, axis=-1, keepdims=True) / width
    centered = values - mean_val
    var_val = jnp.sum(centered * centered, axis=-1, keepdims=True) / width
    inv_std = lax.rsqrt(var_val + EPS)
    standard = centered * inv_std
    return standard * gain + shift, standard, inv_std


def norm_backward(grad_out, gain, standard, inv_std):
    width = grad_out.shape[-1]
    grad_std = grad_out * gain
    m0 = jnp.sum(grad_std, axis=-1, keepdims=True) / width
    m1 = jnp.sum(grad_std * standard, axis=-1, keepdims=True) / width
    return inv_std * (grad_std - m0 - standard * m1)


def gelu_grad(pre_act, grad_out):
    return jax.vjp(jax.nn.gelu, pre_act)[1](grad_out)[0]


def weight_specs():
    vec_spec = P(CHANNEL_AXES)
    layer_vec = P(None, CHANNEL_AXES)
    return (P('fsdp', 'tp'), vec_spec, layer_vec, layer_vec, P(None, None, 'fsdp'), P(None, 'fsdp'),
            P(None, 'fsdp', None), layer_vec, layer_vec, P(None, 'fsdp', 'tp'), layer_vec,
            P(None, CHANNEL_AXES, None), layer_vec, vec_spec, vec_spec, P('fsdp', 'tp'), P('tp'))


def solution(mesh):
    fsdp_size = mesh.shape['fsdp']
    tp_size = mesh.shape['tp']

    def step(patches, labels, w_stem, b_stem, ln1_g, ln1_b, w_tok1, b_tok1, w_tok2,
             ln2_g, ln2_b, w_ch1, b_ch1, w_ch2, b_ch2, lnf_g, lnf_b, w_head, b_head):
        layers = w_tok1.shape[0]
        images = patches.shape[0] // tp_size
        tokens = patches.shape[1]
        channels = w_stem.shape[1] * tp_size
        hidden = w_ch1.shape[2] * tp_size
        tok_hidden = w_tok1.shape[2] * fsdp_size
        classes = w_head.shape[1] * tp_size
        total_images = images * tp_size * fsdp_size
        rows = images * tokens
        z_idx, f_idx = lax.axis_index('tp'), lax.axis_index('fsdp')

        stem_move, stem_windows = stem_pieces(w_stem.astype(BF))
        stem_move.launch()
        width = b_stem.shape[0]
        thin = [b_stem, ln1_g, ln1_b, ln2_g, ln2_b, b_ch2, lnf_g, lnf_b, b_tok1, w_tok1, jnp.swapaxes(w_tok2, 1, 2),
                b_ch1, jnp.pad(b_head, (0, 512 - b_head.shape[0]))]
        thin = jnp.concatenate([v.reshape(-1, width) for v in thin])[None, None, None, None]
        half = classes // tp_size
        head = jnp.pad(w_head.astype(BF), ((0, 0), (0, 512 - half)))
        layer_moves = [layer_pieces(w_ch1[i].astype(BF), w_ch2[i].astype(BF), head if i == layers - 1 else None)
                       for i in range(layers)]
        mine = lax.dynamic_slice_in_dim(patches, z_idx * images, images, 0)
        mine = jnp.transpose(mine, (1, 0, 2)).reshape(rows, -1)
        my_labels = lax.dynamic_slice_in_dim(labels, z_idx * images, images, 0)
        thin = merge_absolute(thin, 'x')
        thin = fence(thin, stem_move)
        thin = merge_absolute(thin, 'y')
        thin = fence(thin, stem_move)
        thin = merge_absolute(thin, 'z')
        move, windows = layer_moves[0]
        move.replace([gate(v, stem_move.held) for v in move.held])
        move.launch()
        thin = merge_absolute(thin, 'core').reshape((16,) + thin.shape[4:])
        flat = jnp.transpose(thin, (1, 0, 2)).reshape(thin.shape[1], -1)
        row = lambda i: flat[i:i + 1]
        stem_bias = row(0)
        ln1_gain, ln1_shift, ln2_gain, ln2_shift, ch_bias2 = [[row(1 + 2 * k + i) for i in range(layers)]
                                                             for k in range(5)]
        lnf_gain, lnf_shift = row(11), row(12)
        at = 13
        tok_bias = [flat[at + i, :tok_hidden].reshape(tok_hidden, 1) for i in range(layers)]
        at += layers
        tok = flat[at:at + 2 * layers * tokens, :tok_hidden].astype(BF).reshape(2, layers, tokens, tok_hidden)
        tok_w1, tok_w2t = tok[0], tok[1]
        at += 2 * layers * tokens
        sub = b_ch1.shape[1] // width
        ch_bias1 = jnp.transpose(flat[at:at + layers * sub].reshape(layers, sub, 16, width), (0, 2, 1, 3)).reshape(
            layers, hidden)
        at += layers * sub
        head_bias = jnp.concatenate([thin[0, at:].reshape(-1)[:classes // 2], thin[8, at:].reshape(-1)[:classes // 2]])

        stem_full = assemble(stem_move.finish(), stem_windows, [(w_stem.shape[0] * 8, channels)], 'put_stem')[0]
        stem_full = fence(stem_full, move)
        mine_sib = exchange(gate(mine, stem_full), 'core')

        def to_rows(v):
            return jnp.transpose(v, (1, 0, 2)).reshape(rows, channels)

        def to_images(v):
            return jnp.transpose(v.reshape(tokens, images, channels), (1, 0, 2))

        resid = to_images(product('rp,pc->rc', mine, stem_full) + stem_bias)
        saved = []
        for layer in range(layers):
            move, windows = layer_moves[layer]
            x_in = resid = fence(resid, move)
            mid, full_in = token_forward(x_in, ln1_gain[layer], ln1_shift[layer], ln2_gain[layer], ln2_shift[layer],
                                         tok_w1[layer], tok_bias[layer], tok_w2t[layer])
            full_in = to_rows(full_in)
            shapes = [(channels, hidden), (hidden, channels)] + ([(channels, 1024)] if layer == layers - 1 else [])
            arrays = move.finish(full_in)
            if layer + 1 < layers:
                after = layer_moves[layer + 1][0]
                after.replace([gate(v, arrays) for v in after.held])
                after.launch()
            ch_w1, ch_w2, *rest = assemble(arrays, windows, shapes, 'put_layer')
            if layer + 1 < layers:
                ch_w1 = fence(ch_w1, after)
            ch_pre = product('rc,cd->rd', full_in, ch_w1) + ch_bias1[layer]
            ch_act = jax.nn.gelu(ch_pre).astype(BF)
            out = product('rd,dc->rc', ch_act, ch_w2) + ch_bias2[layer]
            resid = mid + to_images(out)
            saved.append(dict(x_in=x_in, mid=mid, full_in=full_in, ch_pre=ch_pre, ch_act=ch_act, w1=ch_w1, w2=ch_w2,
                              full_in_sib=exchange(full_in, 'core'), ch_act_sib=exchange(ch_act, 'core')))
        head_w = rest[0]

        pooled = jnp.mean(resid, axis=1)
        head_in, head_std, head_inv = norm_forward(pooled, lnf_gain, lnf_shift)
        head_in = head_in.astype(BF)
        logits = product('bc,ck->bk', head_in, head_w)
        logits = jnp.concatenate([logits[:, :half], logits[:, 512:512 + half]], axis=1) + head_bias
        is_label = jnp.arange(classes)[None, :] == my_labels[:, None]
        row_max = jnp.max(logits, axis=1, keepdims=True)
        shifted = jnp.exp(logits - row_max)
        class_sum = jnp.sum(shifted, axis=1, keepdims=True)
        log_norm = row_max + jnp.log(class_sum)
        loss_part = jnp.sum(log_norm[:, 0] - jnp.sum(jnp.where(is_label, logits, 0.0), axis=1)) / total_images
        d_logits = (shifted / class_sum - is_label.astype(F32)) / total_images
        d_wide = jnp.pad(d_logits.reshape(images, tp_size, half), ((0, 0), (0, 0), (0, 512 - half))).reshape(images, 1024)
        d_logits_bf = d_wide.astype(BF)
        d_head_in = product('bk,ck->bc', d_logits_bf, head_w)
        d_pooled = norm_backward(d_head_in, lnf_gain, head_std, head_inv)
        d_resid = jnp.broadcast_to((d_pooled / tokens)[:, None], (images, tokens, channels))
        d_out = to_rows(d_resid.astype(BF))
        d_sum = jnp.sum(d_pooled, axis=0, keepdims=True)

        big = [None] * layers
        packed = [None] * layers
        pad_row = lambda v: jnp.pad(v.reshape(1, -1), ((0, 0), (0, channels - v.size)))
        extra = [jnp.sum(d_head_in * head_std, axis=0, keepdims=True), jnp.sum(d_head_in, axis=0, keepdims=True),
                 pad_row(jnp.sum(d_logits, axis=0)), pad_row(loss_part)]
        both = Doubling(jnp.concatenate([head_in, d_logits_bf], axis=1)[None], True)
        older, spread = [], [both]
        for layer in reversed(range(layers)):
            keep = saved[layer]
            d_out_sib = exchange(d_out, 'core')
            d_ch_pre = gelu_grad(keep['ch_pre'], product('rc,dc->rd', d_out, keep['w2']))
            g_b_ch1 = jnp.sum(d_ch_pre, axis=0)
            d_ch_pre = d_ch_pre.astype(BF)
            d_ch_pre = fence(d_ch_pre, *spread)
            d_ch_pre_sib = exchange(d_ch_pre, 'core')
            d_norm2 = to_images(product('rd,cd->rc', d_ch_pre, keep['w1']))
            d_norm2 = fence(d_norm2, *older, *spread)
            grads = layer_grad(keep['ch_act'], keep['ch_act_sib'], gate(d_out, d_norm2), d_out_sib,
                               keep['full_in'], keep['full_in_sib'], d_ch_pre, d_ch_pre_sib,
                               w_ch1.shape[1], w_ch1.shape[2], w_ch2.shape[1], channels)
            d_norm2 = fence(d_norm2, grads, *spread)
            more = jnp.concatenate([d_sum, g_b_ch1.reshape(-1, channels)] + extra)
            more = jnp.pad(more, ((0, 16 - more.shape[0]), (0, 0)))
            d_resid, d_out, pack = token_backward(
                keep['x_in'], keep['mid'], d_resid, d_norm2, ln1_gain[layer], ln1_shift[layer], ln2_gain[layer],
                tok_w1[layer], tok_bias[layer], tok_w2t[layer], more)
            d_sum = pack[4:5]
            packed[layer] = Doubling(pack, False)
            extra = []
            d_out = to_rows(d_out)
            for t in older:
                d_out = t.close(d_out)
            d_out = fence(d_out, grads, *[t for t in spread if t.stage < 4])
            big[layer] = grads
            older, spread = [grads], [packed[layer]]

        small_sum = packed[0]
        d_out = fence(d_out, small_sum)
        stem_move = stem_grad(mine, mine_sib, d_out, exchange(d_out, 'core'), w_stem.shape[0], w_stem.shape[1])
        done = fence(jnp.zeros((8, 128), F32), stem_move, small_sum)
        done = fence(done, older[0], small_sum)
        done = fence(done, stem_move, small_sum)
        done = fence(done, stem_move)
        done = older[0].close(done)
        for t in packed + [both]:
            t.got = gate(t.got, done)
            t.fold()
        stem_move.close(done)
        packed = [t.value for t in packed]
        both = both.value.reshape(total_images, -1)
        grad_w1, grad_w2 = zip(*[split_layer_grad(t.done) for t in big])

        head_rows = w_head.shape[0]
        d_cols = lax.dynamic_slice_in_dim(both, channels + z_idx * 512, half, 1)
        g_w_head = product('bc,bk->ck', lax.dynamic_slice_in_dim(both, f_idx * head_rows, head_rows, 1), d_cols)

        dev = z_idx * fsdp_size + f_idx
        own_vec = [lax.dynamic_slice_in_dim(v, dev * width, width, 1) for v in packed]

        def vec_out(k):
            return jnp.stack([v[k] for v in own_vec])

        def chan_out(v):
            n = hidden // 16
            per = channels // n
            return lax.dynamic_slice(v, (65 + dev // per, (dev % per) * n), (1, n))[0]

        tok_n = tok_hidden // fsdp_size
        tok_lo = [lax.dynamic_slice_in_dim(v[5:8 + tokens], f_idx * tok_n, tok_n, 1) for v in packed]
        tok_hi = [lax.dynamic_slice_in_dim(v[8:8 + tokens], tok_hidden + f_idx * tok_n, tok_n, 1) for v in packed]
        last = 65 + hidden // channels
        return (packed[1][last + 3, 0], jnp.concatenate(stem_move.done), own_vec[0][4], vec_out(0), vec_out(1),
                jnp.stack([v[3:] for v in tok_lo]), jnp.stack([v[0] for v in tok_lo]),
                jnp.stack([v.T for v in tok_hi]), vec_out(2), vec_out(3),
                jnp.stack(grad_w1), jnp.stack([chan_out(v) for v in packed]),
                jnp.stack(grad_w2), vec_out(64),
                own_vec[1][last], own_vec[1][last + 1], g_w_head,
                lax.dynamic_slice_in_dim(packed[1][last + 2], z_idx * half, half, 0))

    specs = weight_specs()
    return jax.shard_map(step, mesh=mesh, in_specs=(P('fsdp', None, None), P('fsdp')) + specs,
                         out_specs=(P(),) + specs, check_vma=False)
```
